256 devices in a mesh: chan: 64 (over y, z, core), slot: 4 (over x).
Axes of the slice: x: 4, y: 4, z: 8, core: 2. Of those that a mesh axis runs over, the one named last changes fastest.
Arguments:
- visibility: float32 [2, 2, 256, 4, 3844], P(None, None, 'chan', 'slot'), parts along dimension 3, may hold values from -6 to 6
- coherency: bfloat16 [2, 2, 16, 256, 4, 3844], P(None, None, None, 'chan', 'slot'), parts along dimension 4, may hold values from -2 to 2
- jones_start: float32 [2, 2, 64, 256, 62], P(None, None, 'slot', 'chan'), parts along dimension 2, may hold values from -4 to 4
- duals_start: float32 [2, 2, 64, 256, 62], P(None, None, 'slot', 'chan'), parts along dimension 2, may hold values from -2 to 2
Outputs:
- jones_final: float32 [2, 2, 64, 256, 62], P(None, None, 'slot', 'chan'), parts along dimension 2
- consensus: float32 [2, 2, 64, 256, 62], P(None, None, 'slot', 'chan'), parts along dimension 2
- duals_final: float32 [2, 2, 64, 256, 62], P(None, None, 'slot', 'chan'), parts along dimension 2
- norms: float32 [8, 2], P('slot'), parts along dimension 0
The draws below stay inside these ranges and needn't reach their ends.
There are 4 independent parts, one for each index of `slot`. The reference program is written for one: setup_inputs(seed, part) draws one part's arguments, and reference() takes and returns one part's arrays. A program takes and returns all parts, laid end to end along the dimension named above; each array names one. Nothing has to cross between parts.
All inputs are finite; a program needn't handle non-finite values.
Results may differ from the reference program's by a relative error of at most 0.0003.
Values sent between devices are 32-bit elements; how exact they have to be, the bound alone decides.
No kernel may reach another device: no remote copies, remote signals or barrier semaphores. Data moves between devices by JAX's collectives and lax.ppermute only.
A program may use at most 128 MiB of HBM per device.

```python
import jax
import jax.numpy as jnp
from jax import lax

STATIONS = 62
DIRS = 16
POLS = 2
TIMES = 1
ITERS = 2
CH_DEV = 4
CHANNELS = 256
PAIRS = 3844
N_CHAN = 64


def block_levels(key, extent, cuts, low, high):
    def one(dim, shards_of):
        heights = jax.random.uniform(jax.random.fold_in(jax.random.fold_in(key, 6), dim), (shards_of,), jnp.float32, low / len(cuts), high / len(cuts))
        return jnp.repeat(jnp.exp(heights), extent[dim] // shards_of).reshape((-1,) + (1,) * (len(extent) - dim - 1))

    level = one(*cuts[0])
    for cut in cuts[1:]:
        level = level * one(*cut)
    return level


def scatter_about(rng, dims, scale, bound, split=(), kind=jnp.bfloat16):
    values = jax.random.normal(rng, dims, jnp.float32) * scale
    if len(split) > 0:
        values = block_levels(rng, dims, split, -0.22, 0.18) * values
    return jnp.clip(values, min=-bound, max=bound).astype(kind)


def setup_inputs(seed: int = 0, part: int = 0) -> dict:
    key_list = jax.random.split(jax.random.key(seed), 5)
    part_splits = jax.random.split(jax.random.fold_in(key_list[4], part), 5)
    visibility = scatter_about(part_splits[0], (2, POLS, CHANNELS, TIMES, PAIRS), 1.0, 6.0, ((2, 64),), jnp.float32)
    coherency = scatter_about(part_splits[1], (2, POLS, DIRS, CHANNELS, TIMES, PAIRS), 0.25, 2.0, ((3, 64),))
    jones_start = scatter_about(part_splits[2], (2, POLS, DIRS, CHANNELS, STATIONS), 0.7, 4.0, ((3, 64),), jnp.float32)
    duals_start = scatter_about(part_splits[3], (2, POLS, DIRS, CHANNELS, STATIONS), 0.3, 2.0, ((3, 64),), jnp.float32)
    return {"visibility": visibility, "coherency": coherency, "jones_start": jones_start, "duals_start": duals_start}


penalty = 8.0
kernel_taps = (0.04, 0.06, 0.1, 0.15, 0.3, 0.15, 0.1, 0.06, 0.04)


def jones_update(visibility, coherency, jones_now, target):
    width = jones_now.shape[-1]
    grid_shape = coherency.shape[1:5] + (width, width)
    sky_real = coherency[0].astype(jnp.float32).reshape(grid_shape)
    sky_imag = coherency[1].astype(jnp.float32).reshape(grid_shape)
    vis_shape = visibility.shape[1:4] + (width, width)
    data_real = visibility[0].reshape(vis_shape)[:, None]
    data_imag = visibility[1].reshape(vis_shape)[:, None]
    left_real = jones_now[0][:, :, :, None, :, None]
    left_imag = jones_now[1][:, :, :, None, :, None]
    right_real = jones_now[0][:, :, :, None, None, :]
    right_imag = jones_now[1][:, :, :, None, None, :]
    crossed = 1.0 - jnp.eye(width, dtype=jnp.float32)
    half_real = left_real * sky_real - left_imag * sky_imag
    half_imag = left_real * sky_imag + left_imag * sky_real
    model_real = half_real * right_real + half_imag * right_imag
    model_imag = half_imag * right_real - half_real * right_imag
    rest_real = (data_real - jnp.sum(model_real, axis=1, keepdims=True) + model_real) * crossed
    rest_imag = (data_imag - jnp.sum(model_imag, axis=1, keepdims=True) + model_imag) * crossed
    weight_real = sky_real * right_real + sky_imag * right_imag
    weight_imag = sky_real * right_imag - sky_imag * right_real
    upper_real = jnp.sum(rest_real * weight_real - rest_imag * weight_imag, axis=(3, 5))
    upper_imag = jnp.sum(rest_real * weight_imag + rest_imag * weight_real, axis=(3, 5))
    lower = jnp.sum(crossed * (sky_real * sky_real + sky_imag * sky_imag) * (right_real * right_real + right_imag * right_imag), axis=(3, 5)) + penalty
    return jnp.stack([(upper_real + penalty * target[0]) / lower, (upper_imag + penalty * target[1]) / lower])


def blocked_update(visibility, coherency, jones_now, target):
    vis_shape = visibility.shape
    vis_blocks = jnp.moveaxis(visibility.reshape(vis_shape[:2] + (N_CHAN, CH_DEV) + vis_shape[3:]), 2, 0)
    coh_shape = coherency.shape
    coh_blocks = jnp.moveaxis(coherency.reshape(coh_shape[:3] + (N_CHAN, CH_DEV) + coh_shape[4:]), 3, 0)
    gain_shape = jones_now.shape
    gain_blocks = jnp.moveaxis(jones_now.reshape(gain_shape[:3] + (N_CHAN, CH_DEV) + gain_shape[4:]), 3, 0)
    target_blocks = jnp.moveaxis(target.reshape(gain_shape[:3] + (N_CHAN, CH_DEV) + gain_shape[4:]), 3, 0)
    updated = lax.map(lambda blocks_in: jones_update(*blocks_in), (vis_blocks, coh_blocks, gain_blocks, target_blocks))
    return jnp.moveaxis(updated, 0, 3).reshape(gain_shape)


def smooth(padded, channels):
    total = kernel_taps[0] * padded[:, :, :, 0:channels]
    for offset in range(1, 9):
        total = total + kernel_taps[offset] * padded[:, :, :, offset:offset + channels]
    return total


def reference(visibility, coherency, jones_start, duals_start):
    channels = jones_start.shape[3]
    entries = jones_start.size
    jones_now = jones_start
    consensus = jones_start
    duals_now = duals_start
    partials = []
    for iteration in range(ITERS):
        jones_now = blocked_update(visibility, coherency, jones_now, consensus - duals_now)
        summed = jones_now + duals_now
        padded = jnp.pad(summed, ((0, 0), (0, 0), (0, 0), (4, 4), (0, 0)))
        fresh = smooth(padded, channels)
        duals_now = duals_now + jones_now - fresh
        primal_gap = jones_now - fresh
        moved = fresh - consensus
        primal = jnp.sum(primal_gap * primal_gap) / entries
        change = penalty * penalty * jnp.sum(moved * moved) / entries
        partials.append(jnp.stack([primal, change]))
        consensus = fresh
    return jones_now, consensus, duals_now, jnp.stack(partials)
```

```python
import jax
import jax.numpy as jnp
from jax import lax
from jax.experimental import pallas as pl
from jax.experimental.pallas import tpu as pltpu
from jax.sharding import PartitionSpec as P

penalty = 8.0
kernel_taps = (0.04, 0.06, 0.1, 0.15, 0.3, 0.15, 0.1, 0.06, 0.04)
N = 62
M = 64
LANES = 128
PAIRS = N * N
F32 = jnp.float32
BF16 = jnp.bfloat16
GROUP = 4


def iota(shape, dim):
    return lax.broadcasted_iota(jnp.int32, shape, dim)


def rows_first(ref, out_rows=M):
    halves = []
    for part in range(2):
        x = jnp.concatenate([ref[part, pol, k] for pol in range(2) for k in range(16)], axis=0)
        x = jnp.concatenate([x, jnp.zeros((LANES, LANES - N), F32)], axis=1)
        halves.append(x.T[:out_rows])
    return jnp.concatenate(halves, axis=1)


def rows_last(x, ref):
    for part in range(2):
        half = x[:, part * LANES : (part + 1) * LANES]
        half = jnp.concatenate([half, jnp.zeros((LANES - M, LANES), F32)], axis=0).T
        for pol in range(2):
            for k in range(16):
                at = (pol * 16 + k) * 4
                ref[part, pol, k] = half[at : at + 4, :N]


def lay_out(coh_ref, vis_ref, flat, vflat, ct, vt):
    width = 31 * LANES
    flat[:, width - LANES :] = jnp.zeros((256, LANES), BF16)
    vflat[:, width - LANES :] = jnp.zeros((48, LANES), BF16)
    for part in range(2):
        for pol in range(2):
            for k in range(0, 16, 4):
                at = part * 128 + pol * 64 + k * 4
                block = [coh_ref[part, pol, k + i].astype(F32) for i in range(4)]
                flat[at : at + 16, :PAIRS] = jnp.concatenate(block, axis=0).astype(BF16)
    v = jnp.concatenate([vis_ref[part, pol] for part in range(2) for pol in range(2)], axis=0)
    for split in range(3):
        high = v.astype(BF16)
        vflat[split * 16 : split * 16 + 16, :PAIRS] = high
        v = v - high.astype(F32)
    row = iota((128, 256), 0)
    col = iota((128, 256), 1)
    half = row // M
    q = row % M
    lag = jnp.where(q < N, col - half * N - q, 1000)
    own = q - half
    source = iota((48, 256), 0)
    target = iota((48, 256), 1)
    spread = (
        ((source % 16) // 8 == target // LANES)
        & ((source % 8) // 4 == (target % LANES) // 64)
        & (source % 4 == target % 4)
    )
    spread = jnp.where(spread, 1.0, 0.0).astype(BF16)
    for t in range(31):
        start = 124 * t // LANES * LANES
        shift = 124 * t - start
        pick = jnp.where((lag == shift) & (own != 2 * t), 1.0, 0.0).astype(BF16)
        contract = (((1,), (1,)), ((), ()))
        ct[t * 128 : t * 128 + 128] = lax.dot_general(
            pick, flat[:, start : start + 256], contract, preferred_element_type=F32
        )
        short = lax.dot_general(
            pick, vflat[:, start : start + 256], contract, preferred_element_type=F32
        )
        vt[t * 128 : t * 128 + 128] = jnp.dot(
            short.astype(BF16), spread, preferred_element_type=F32
        )
    ct[31 * 128 :] = jnp.zeros((128, 256), F32)
    vt[31 * 128 :] = jnp.zeros((128, 256), F32)


def pair_sums(ct, vt, gain, total, weight, lhs, half, model):
    row = iota((256, LANES), 0) % LANES
    col = iota((256, LANES), 1)
    same = (row // 64 == col // 64) & (row % 4 == col % 4)
    adder = jnp.where(same, 1.0, 0.0).astype(BF16)

    def front(group):
        slot = group % 2
        for i in range(GROUP):
            p = group * GROUP + i
            c_real = ct[p * M : p * M + M, :LANES]
            c_imag = ct[p * M : p * M + M, LANES:]
            q_real = gain[:, :LANES]
            q_imag = gain[:, LANES:]
            h_real = c_real * q_real + c_imag * q_imag
            h_imag = c_imag * q_real - c_real * q_imag
            p_real = gain[p : p + 1, :LANES]
            p_imag = gain[p : p + 1, LANES:]
            half[slot, i * M : i * M + M, :LANES] = h_real
            half[slot, i * M : i * M + M, LANES:] = h_imag
            for at, m in (
                (i * 128, p_real * h_real - p_imag * h_imag),
                (i * 128 + M, p_real * h_imag + p_imag * h_real),
            ):
                high = m.astype(BF16)
                lhs[slot, at : at + M, :LANES] = high
                lhs[slot, at : at + M, LANES:] = (m - high.astype(F32)).astype(BF16)
        model[slot] = jnp.dot(lhs[slot], adder, preferred_element_type=F32)

    def back(group):
        slot = group % 2
        for i in range(GROUP):
            p = group * GROUP + i
            h_real = half[slot, i * M : i * M + M, :LANES]
            h_imag = half[slot, i * M : i * M + M, LANES:]
            d_real = vt[p * M : p * M + M, :LANES] - model[slot, i * 128 : i * 128 + M]
            d_imag = vt[p * M : p * M + M, LANES:] - model[slot, i * 128 + M : i * 128 + 128]

            def over_q(x):
                return jnp.sum(x, axis=0, keepdims=True)

            total[p : p + 1, :LANES] = over_q(d_real * h_real + d_imag * h_imag)
            total[p : p + 1, LANES:] = over_q(d_imag * h_real - d_real * h_imag)
            weight[p : p + 1] = over_q(h_real * h_real + h_imag * h_imag)

    front(0)
    for group in range(M // GROUP):
        if group + 1 < M // GROUP:
            front(group + 1)
        back(group)


def solved(total, weight, gain, target):
    twice = jnp.concatenate([weight, weight], axis=1)
    return (total + gain * twice + penalty * target) / (twice + penalty)


def first_kernel(
    coh_ref, vis_ref, jones_ref, duals_ref,
    sum_ref, gain_ref, start_ref, duals_out, ct, vt,
    flat, vflat, total, weight, lhs, half, model,
):
    lay_out(coh_ref, vis_ref, flat, vflat, ct, vt)
    start_ref[...] = rows_first(jones_ref)
    duals_out[...] = rows_first(duals_ref)
    pair_sums(ct, vt, start_ref, total, weight, lhs, half, model)
    gain = solved(total[...], weight[...], start_ref[...], start_ref[...] - duals_out[...])
    gain_ref[...] = gain
    sum_ref[...] = gain + duals_out[...]


def second_kernel(ct, vt, gain_ref, total, weight, lhs, half, model):
    pair_sums(ct, vt, gain_ref, total, weight, lhs, half, model)


def smoothed(odd, own, inner, outer):
    source = iota((LANES, LANES), 0)
    target = iota((LANES, LANES), 1)
    lag = jnp.where(source // 4 == target // 4, source % 4 - target % 4, 100)

    def taps(shift):
        out = jnp.zeros((LANES, LANES), F32)
        for offset in range(-4, 5):
            out = jnp.where(lag + shift == offset, kernel_taps[offset + 4], out)
        return out

    after, before = taps(4), taps(-4)
    weights = jnp.concatenate(
        [taps(0), jnp.where(odd, before, after), jnp.where(odd, after, before)], axis=0
    )
    halves = []
    for part in range(2):
        x = jnp.concatenate(
            [a[:, part * LANES : (part + 1) * LANES] for a in (own, inner, outer)], axis=1
        )
        halves.append(
            jnp.dot(x, weights, precision=lax.Precision.HIGHEST, preferred_element_type=F32)
        )
    return jnp.concatenate(halves, axis=1)


def gaps(gain, fresh, consensus):
    primal = gain - fresh
    moved = fresh - consensus
    return (
        jnp.sum(primal * primal, keepdims=True),
        penalty * penalty * jnp.sum(moved * moved, keepdims=True),
    )


def third_kernel(
    odd_ref, own_ref, inner_ref, outer_ref, gain_ref, start_ref, duals_ref, total, weight,
    sum_ref, gain_out, fresh_ref, duals_out, norms_ref,
):
    fresh = smoothed(odd_ref[0] == 1, own_ref[...], inner_ref[...], outer_ref[...])
    gain = gain_ref[...]
    duals = duals_ref[...] + gain - fresh
    first, second = gaps(gain, fresh, start_ref[...])
    gain = solved(total[...], weight[...], gain, fresh - duals)
    gain_out[...] = gain
    fresh_ref[...] = fresh
    duals_out[...] = duals
    sum_ref[...] = gain + duals
    lane = iota((1, LANES), 1)
    norms_ref[...] = jnp.where(lane == 0, first, jnp.where(lane == 1, second, 0.0))


def fourth_kernel(
    odd_ref, own_ref, inner_ref, outer_ref, gain_ref, fresh_ref, duals_ref, norms_ref,
    fresh_out, duals_out, norms_out,
):
    fresh = smoothed(odd_ref[0] == 1, own_ref[...], inner_ref[...], outer_ref[...])
    gain = gain_ref[...]
    duals = duals_ref[...] + gain - fresh
    first, second = gaps(gain, fresh, fresh_ref[...])
    lane = iota((1, LANES), 1)
    norms = norms_ref[...] + jnp.where(lane == 2, first, jnp.where(lane == 3, second, 0.0))
    norms_out[...] = jnp.broadcast_to(norms[None], norms_out.shape)
    rows_last(fresh, fresh_out)
    rows_last(duals, duals_out)


def turn_kernel(gain_ref, out_ref):
    rows_last(gain_ref[...], out_ref)


def call(kernel, outs, ins, scratch=(), smem=(), flops=0):
    return pl.pallas_call(
        kernel,
        out_shape=[jax.ShapeDtypeStruct(shape, F32) for shape in outs],
        in_specs=[
            pl.BlockSpec(memory_space=pltpu.SMEM if i in smem else pltpu.VMEM)
            for i in range(len(ins))
        ],
        out_specs=[pl.BlockSpec(memory_space=pltpu.VMEM) for _ in outs],
        scratch_shapes=scratch,
        cost_estimate=pl.CostEstimate(flops=flops, bytes_accessed=1000, transcendentals=0),
        compiler_params=pltpu.CompilerParams(vmem_limit_bytes=48 * 1024 * 1024),
        name=kernel.__name__,
    )(*ins)


def local(visibility, coherency, jones_start, duals_start):
    cards = lax.axis_size("chan")
    entries = jones_start.size * cards
    odd = (lax.axis_index("chan") % 2).astype(jnp.int32).reshape(1)
    inner = [(i, i ^ 1) for i in range(cards)]
    outer = [(i, i - 1 if i % 2 == 0 else i + 1) for i in range(cards)]
    outer = [(a, b) for a, b in outer if 0 <= b < cards]
    state = (M, 2 * LANES)
    work = [
        pltpu.VMEM((2, GROUP * 128, 256), BF16),
        pltpu.VMEM((2, GROUP * M, 256), F32),
        pltpu.VMEM((2, GROUP * 128, LANES), F32),
    ]
    sums, gain, start, duals, ct, vt = call(
        first_kernel,
        [state, state, state, state, (M * M, 256), (M * M, 256)],
        (
            coherency.reshape(2, 2, 16, 4, PAIRS),
            visibility.reshape(2, 2, 4, PAIRS),
            jones_start,
            duals_start,
        ),
        [
            pltpu.VMEM((256, 31 * LANES), BF16),
            pltpu.VMEM((48, 31 * LANES), BF16),
            pltpu.VMEM(state, F32),
            pltpu.VMEM((M, LANES), F32),
            *work,
        ],
        flops=10**10,
    )

    def swapped(x):
        return lax.ppermute(x, "chan", inner), lax.ppermute(x, "chan", outer)

    near, far = swapped(sums)
    total, weight = call(
        second_kernel, [state, (M, LANES)], (ct, vt, gain), work, flops=10**10
    )
    sums, gain, fresh, duals, norms = call(
        third_kernel,
        [state, state, state, state, (1, LANES)],
        (odd, sums, near, far, gain, start, duals, total, weight),
        smem=(0,),
    )
    near, far = swapped(sums)
    shape = jones_start.shape
    (jones_now,) = call(turn_kernel, [shape], (gain,), flops=10**9)
    consensus, duals_now, norms = call(
        fourth_kernel,
        [shape, shape, (cards, 1, LANES)],
        (odd, sums, near, far, gain, fresh, duals, norms),
        smem=(0,),
    )
    norms = lax.all_to_all(norms, "chan", split_axis=0, concat_axis=0, tiled=True)
    norms = jnp.sum(norms[:, 0, :4], axis=0).reshape(2, 2) / entries
    return jones_now, consensus, duals_now, norms


def solution(mesh):
    placed = (
        P(None, None, "chan", "slot", None),
        P(None, None, None, "chan", "slot", None),
        P(None, None, "slot", "chan", None),
        P(None, None, "slot", "chan", None),
    )
    return jax.shard_map(
        local,
        mesh=mesh,
        in_specs=placed,
        out_specs=(
            P(None, None, "slot", "chan", None),
            P(None, None, "slot", "chan", None),
            P(None, None, "slot", "chan", None),
            P("slot", None),
        ),
        check_vma=False,
    )
```

```python
import jax
import jax.numpy as jnp
from jax import lax
from jax.experimental import pallas as pl
from jax.experimental.pallas import tpu as pltpu
from jax.sharding import PartitionSpec as P

penalty = 8.0
kernel_taps = (0.04, 0.06, 0.1, 0.15, 0.3, 0.15, 0.1, 0.06, 0.04)
N = 62
M = 64
LANES = 128
PAIRS = N * N
F32 = jnp.float32
BF16 = jnp.bfloat16
ROWS = 31 * LANES
GROUP = 4


def iota(shape, dim):
    return lax.broadcasted_iota(jnp.int32, shape, dim)


def rows_first(ref, out_rows=M):
    halves = []
    for part in range(2):
        x = jnp.concatenate([ref[part, pol, k] for pol in range(2) for k in range(16)], axis=0)
        x = jnp.concatenate([x, jnp.zeros((LANES, LANES - N), F32)], axis=1)
        halves.append(x.T[:out_rows])
    return jnp.concatenate(halves, axis=1)


def rows_last(x, ref):
    for part in range(2):
        half = x[:, part * LANES : (part + 1) * LANES]
        half = jnp.concatenate([half, jnp.zeros((LANES - M, LANES), F32)], axis=0).T
        for pol in range(2):
            for k in range(16):
                at = (pol * 16 + k) * 4
                ref[part, pol, k] = half[at : at + 4, :N]


def lay_out(coh_ref, vis_ref, vflat, short, ct, vt, copies):
    vflat[:, ROWS - LANES :] = jnp.zeros((48, LANES), BF16)
    copies[0].wait()
    v = jnp.concatenate(
        [vis_ref[a, b, f] for a in range(2) for b in range(2) for f in range(4)], axis=0
    )
    for split in range(3):
        high = v.astype(BF16)
        vflat[split * 16 : split * 16 + 16, :PAIRS] = high
        v = v - high.astype(F32)
    same = jnp.where(iota((LANES, LANES), 0) == iota((LANES, LANES), 1), 1.0, 0.0).astype(BF16)
    for start in range(0, ROWS, LANES):
        short[start : start + LANES] = lax.dot_general(
            same,
            vflat[:, start : start + LANES],
            (((1,), (1,)), ((), ())),
            preferred_element_type=F32,
        ).astype(BF16)
    source = iota((48, 256), 0)
    target = iota((48, 256), 1)
    spread = (
        ((source % 16) // 8 == target // LANES)
        & ((source % 8) // 4 == (target % LANES) // 64)
        & (source % 4 == target % 4)
    )
    spread = jnp.where(spread, 1.0, 0.0).astype(BF16)
    for start in range(0, ROWS, ROWS // 4):
        wide = jnp.dot(
            short[start : start + ROWS // 4], spread, preferred_element_type=F32
        )
        vt[0, start : start + ROWS // 4] = wide[:, :LANES]
        vt[1, start : start + ROWS // 4] = wide[:, LANES:]
    for part in range(2):
        copies[1 + part * 2].wait()
        copies[2 + part * 2].wait()
        for start in range(0, ROWS, LANES):
            x = jnp.concatenate(
                [
                    coh_ref[part, pol, k, :, start : min(start + LANES, PAIRS)].astype(F32)
                    for pol in range(2)
                    for k in range(16)
                ],
                axis=0,
            )
            if x.shape[1] < LANES:
                x = jnp.concatenate([x, jnp.zeros((LANES, LANES - x.shape[1]), F32)], axis=1)
            ct[part, start : start + LANES] = x.T
        for p in range(N):
            ct[part, p * N + p : p * N + p + 1] = jnp.zeros((1, LANES), F32)


def pair_sums(ct, vt, gain, total, weight, lhs, half, model):
    row = iota((256, LANES), 0) % LANES
    col = iota((256, LANES), 1)
    same = (row // 64 == col // 64) & (row % 4 == col % 4)
    adder = jnp.where(same, 1.0, 0.0).astype(BF16)

    def count(group):
        return min(GROUP, N - group * GROUP)

    def front(group):
        slot = group % 2
        for i in range(count(group)):
            p = group * GROUP + i
            c_real = ct[0, p * N : p * N + M]
            c_imag = ct[1, p * N : p * N + M]
            q_real = gain[:, :LANES]
            q_imag = gain[:, LANES:]
            h_real = c_real * q_real + c_imag * q_imag
            h_imag = c_imag * q_real - c_real * q_imag
            p_real = gain[p : p + 1, :LANES]
            p_imag = gain[p : p + 1, LANES:]
            half[slot, i * M : i * M + M, :LANES] = h_real
            half[slot, i * M : i * M + M, LANES:] = h_imag
            for at, m in (
                (i * 128, p_real * h_real - p_imag * h_imag),
                (i * 128 + M, p_real * h_imag + p_imag * h_real),
            ):
                high = m.astype(BF16)
                lhs[slot, at : at + M, :LANES] = high
                lhs[slot, at : at + M, LANES:] = (m - high.astype(F32)).astype(BF16)
        rows = count(group) * 128
        model[slot, :rows] = jnp.dot(lhs[slot, :rows], adder, preferred_element_type=F32)

    def back(group):
        slot = group % 2
        for i in range(count(group)):
            p = group * GROUP + i
            h_real = half[slot, i * M : i * M + M, :LANES]
            h_imag = half[slot, i * M : i * M + M, LANES:]
            d_real = vt[0, p * N : p * N + M] - model[slot, i * 128 : i * 128 + M]
            d_imag = vt[1, p * N : p * N + M] - model[slot, i * 128 + M : i * 128 + 128]

            def over_q(x):
                return jnp.sum(x, axis=0, keepdims=True)

            total[p : p + 1, :LANES] = over_q(d_real * h_real + d_imag * h_imag)
            total[p : p + 1, LANES:] = over_q(d_imag * h_real - d_real * h_imag)
            weight[p : p + 1] = over_q(h_real * h_real + h_imag * h_imag)

    total[N:] = jnp.zeros((M - N, 2 * LANES), F32)
    weight[N:] = jnp.zeros((M - N, LANES), F32)
    front(0)
    for group in range(M // GROUP):
        if group + 1 < M // GROUP:
            front(group + 1)
        back(group)


def solved(total, weight, gain, target):
    twice = jnp.concatenate([weight, weight], axis=1)
    return (total + gain * twice + penalty * target) / (twice + penalty)


def first_kernel(
    coh_hbm, vis_hbm, jones_hbm, duals_hbm,
    sum_ref, gain_ref, start_ref, duals_out, ct, vt,
    coh_ref, vis_ref, jones_ref, duals_ref, vflat, short, total, weight, lhs, half, model, arrived,
):
    copies = [
        pltpu.make_async_copy(source, target, arrived.at[i])
        for i, (source, target) in enumerate(
            [
                (jones_hbm, jones_ref),
                (duals_hbm, duals_ref),
                (vis_hbm, vis_ref),
                *((coh_hbm.at[a, b], coh_ref.at[a, b]) for a in range(2) for b in range(2)),
            ]
        )
    ]
    for copy in copies:
        copy.start()
    copies[0].wait()
    start_ref[...] = rows_first(jones_ref)
    copies[1].wait()
    duals_out[...] = rows_first(duals_ref)
    lay_out(coh_ref, vis_ref, vflat, short, ct, vt, copies[2:])
    pair_sums(ct, vt, start_ref, total, weight, lhs, half, model)
    gain = solved(total[...], weight[...], start_ref[...], start_ref[...] - duals_out[...])
    gain_ref[...] = gain
    sum_ref[...] = gain + duals_out[...]


def second_kernel(ct, vt, gain_ref, total, weight, lhs, half, model):
    pair_sums(ct, vt, gain_ref, total, weight, lhs, half, model)


def smoothed(odd, own, inner, outer):
    source = iota((LANES, LANES), 0)
    target = iota((LANES, LANES), 1)
    lag = jnp.where(source // 4 == target // 4, source % 4 - target % 4, 100)

    def taps(shift):
        out = jnp.zeros((LANES, LANES), F32)
        for offset in range(-4, 5):
            out = jnp.where(lag + shift == offset, kernel_taps[offset + 4], out)
        return out

    after, before = taps(4), taps(-4)
    weights = jnp.concatenate(
        [taps(0), jnp.where(odd, before, after), jnp.where(odd, after, before)], axis=0
    )
    halves = []
    for part in range(2):
        x = jnp.concatenate(
            [a[:, part * LANES : (part + 1) * LANES] for a in (own, inner, outer)], axis=1
        )
        halves.append(
            jnp.dot(x, weights, precision=lax.Precision.HIGHEST, preferred_element_type=F32)
        )
    return jnp.concatenate(halves, axis=1)


def gaps(gain, fresh, consensus):
    primal = gain - fresh
    moved = fresh - consensus
    return (
        jnp.sum(primal * primal, keepdims=True),
        penalty * penalty * jnp.sum(moved * moved, keepdims=True),
    )


def third_kernel(
    odd_ref, own_ref, inner_ref, outer_ref, gain_ref, start_ref, duals_ref, total, weight,
    sum_ref, gain_out, fresh_ref, duals_out, norms_ref,
):
    fresh = smoothed(odd_ref[0] == 1, own_ref[...], inner_ref[...], outer_ref[...])
    gain = gain_ref[...]
    duals = duals_ref[...] + gain - fresh
    first, second = gaps(gain, fresh, start_ref[...])
    gain = solved(total[...], weight[...], gain, fresh - duals)
    gain_out[...] = gain
    fresh_ref[...] = fresh
    duals_out[...] = duals
    sum_ref[...] = gain + duals
    lane = iota((1, LANES), 1)
    norms_ref[...] = jnp.where(lane == 0, first, jnp.where(lane == 1, second, 0.0))


def fourth_kernel(
    odd_ref, own_ref, inner_ref, outer_ref, gain_ref, fresh_ref, duals_ref, norms_ref,
    fresh_out, duals_out, norms_out,
):
    fresh = smoothed(odd_ref[0] == 1, own_ref[...], inner_ref[...], outer_ref[...])
    gain = gain_ref[...]
    duals = duals_ref[...] + gain - fresh
    first, second = gaps(gain, fresh, fresh_ref[...])
    lane = iota((1, LANES), 1)
    norms = norms_ref[...] + jnp.where(lane == 2, first, jnp.where(lane == 3, second, 0.0))
    norms_out[...] = jnp.broadcast_to(norms[None], norms_out.shape)
    fresh_out[...] = fresh
    duals_out[...] = duals


def turn_kernel(*refs):
    for source, target in zip(refs[: len(refs) // 2], refs[len(refs) // 2 :]):
        rows_last(source[...], target)


def call(kernel, outs, ins, scratch=(), smem=(), hbm=(), flops=0):
    def space(i):
        return pltpu.SMEM if i in smem else pltpu.HBM if i in hbm else pltpu.VMEM

    return pl.pallas_call(
        kernel,
        out_shape=[jax.ShapeDtypeStruct(shape, F32) for shape in outs],
        in_specs=[pl.BlockSpec(memory_space=space(i)) for i in range(len(ins))],
        out_specs=[pl.BlockSpec(memory_space=pltpu.VMEM) for _ in outs],
        scratch_shapes=scratch,
        cost_estimate=pl.CostEstimate(flops=flops, bytes_accessed=1000, transcendentals=0),
        compiler_params=pltpu.CompilerParams(vmem_limit_bytes=24 * 1024 * 1024),
        name=kernel.__name__,
    )(*ins)


def local(visibility, coherency, jones_start, duals_start):
    cards = lax.axis_size("chan")
    entries = jones_start.size * cards
    odd = (lax.axis_index("chan") % 2).astype(jnp.int32).reshape(1)
    inner = [(i, i ^ 1) for i in range(cards)]
    outer = [(i, i - 1 if i % 2 == 0 else i + 1) for i in range(cards)]
    outer = [(a, b) for a, b in outer if 0 <= b < cards]
    state = (M, 2 * LANES)
    work = [
        pltpu.VMEM((2, GROUP * 128, 256), BF16),
        pltpu.VMEM((2, GROUP * M, 256), F32),
        pltpu.VMEM((2, GROUP * 128, LANES), F32),
    ]
    sums, gain, start, duals, ct, vt = call(
        first_kernel,
        [state, state, state, state, (2, ROWS, LANES), (2, ROWS, LANES)],
        (
            *(
                pltpu.with_memory_space_constraint(x, pltpu.HBM)
                for x in (
                    coherency.reshape(2, 2, 16, 4, PAIRS), visibility, jones_start, duals_start
                )
            ),
        ),
        [
            pltpu.VMEM((2, 2, 16, 4, PAIRS), BF16),
            pltpu.VMEM(visibility.shape, F32),
            pltpu.VMEM(jones_start.shape, F32),
            pltpu.VMEM(duals_start.shape, F32),
            pltpu.VMEM((48, ROWS), BF16),
            pltpu.VMEM((ROWS, 48), BF16),
            pltpu.VMEM(state, F32),
            pltpu.VMEM((M, LANES), F32),
            *work,
            pltpu.SemaphoreType.DMA((7,)),
        ],
        hbm=(0, 1, 2, 3),
        flops=10**10,
    )

    def swapped(x):
        return lax.ppermute(x, "chan", inner), lax.ppermute(x, "chan", outer)

    near, far = swapped(sums)
    total, weight = call(
        second_kernel, [state, (M, LANES)], (ct, vt, gain), work, flops=10**10
    )
    sums, gain, fresh, duals, norms = call(
        third_kernel,
        [state, state, state, state, (1, LANES)],
        (odd, sums, near, far, gain, start, duals, total, weight),
        smem=(0,),
    )
    near, far = swapped(sums)
    shape = jones_start.shape
    (jones_now,) = call(turn_kernel, [shape], (gain,), flops=10**9)
    fresh, duals, norms = call(
        fourth_kernel,
        [state, state, (cards, 1, LANES)],
        (odd, sums, near, far, gain, fresh, duals, norms),
        smem=(0,),
    )
    consensus, duals_now = call(turn_kernel, [shape, shape], (fresh, duals), flops=10**9)
    norms = lax.all_to_all(norms, "chan", split_axis=0, concat_axis=0, tiled=True)
    norms = jnp.sum(norms[:, 0, :4], axis=0).reshape(2, 2) / entries
    return jones_now, consensus, duals_now, norms


def solution(mesh):
    placed = (
        P(None, None, "chan", "slot", None),
        P(None, None, None, "chan", "slot", None),
        P(None, None, "slot", "chan", None),
        P(None, None, "slot", "chan", None),
    )
    return jax.shard_map(
        local,
        mesh=mesh,
        in_specs=placed,
        out_specs=(
            P(None, None, "slot", "chan", None),
            P(None, None, "slot", "chan", None),
            P(None, None, "slot", "chan", None),
            P("slot", None),
        ),
        check_vma=False,
    )
```

```python
import jax
import jax.numpy as jnp
from jax import lax
from jax.experimental import pallas as pl
from jax.experimental.pallas import tpu as pltpu
from jax.sharding import PartitionSpec as P


penalty = 8.0
kernel_taps = (0.04, 0.06, 0.1, 0.15, 0.3, 0.15, 0.1, 0.06, 0.04)
N = 62
M = 64
LANES = 128
PAIRS = N * N
F32 = jnp.float32
BF16 = jnp.bfloat16
ROWS = 31 * LANES
GROUP = 4


def iota(shape, dim):
    return lax.broadcasted_iota(jnp.int32, shape, dim)


def rows_first(ref, out_rows=M):
    halves = []
    for part in range(2):
        x = jnp.concatenate([ref[part, pol, k] for pol in range(2) for k in range(16)], axis=0)
        x = jnp.concatenate([x, jnp.zeros((LANES, LANES - N), F32)], axis=1)
        halves.append(x.T[:out_rows])
    return jnp.concatenate(halves, axis=1)


def rows_last(x, ref):
    for part in range(2):
        half = x[:, part * LANES : (part + 1) * LANES]
        half = jnp.concatenate([half, jnp.zeros((LANES - M, LANES), F32)], axis=0).T
        for pol in range(2):
            for k in range(16):
                at = (pol * 16 + k) * 4
                ref[part, pol, k] = half[at : at + 4, :N]


def lay_out(coh_ref, vis_ref, vflat, short, ct, vt, copies):
    vflat[:, ROWS - LANES :] = jnp.zeros((48, LANES), BF16)
    copies[0].wait()
    v = jnp.concatenate(
        [vis_ref[a, b, f] for a in range(2) for b in range(2) for f in range(4)], axis=0
    )
    for split in range(3):
        high = v.astype(BF16)
        vflat[split * 16 : split * 16 + 16, :PAIRS] = high
        v = v - high.astype(F32)
    same = jnp.where(iota((LANES, LANES), 0) == iota((LANES, LANES), 1), 1.0, 0.0).astype(BF16)
    for start in range(0, ROWS, LANES):
        short[start : start + LANES] = lax.dot_general(
            same,
            vflat[:, start : start + LANES],
            (((1,), (1,)), ((), ())),
            preferred_element_type=F32,
        ).astype(BF16)
    source = iota((48, 256), 0)
    target = iota((48, 256), 1)
    spread = (
        ((source % 16) // 8 == target // LANES)
        & ((source % 8) // 4 == (target % LANES) // 64)
        & (source % 4 == target % 4)
    )
    spread = jnp.where(spread, 1.0, 0.0).astype(BF16)
    for start in range(0, ROWS, ROWS // 4):
        wide = jnp.dot(
            short[start : start + ROWS // 4], spread, preferred_element_type=F32
        )
        vt[0, start : start + ROWS // 4] = wide[:, :LANES]
        vt[1, start : start + ROWS // 4] = wide[:, LANES:]
    for part in range(2):
        copies[1 + part * 2].wait()
        copies[2 + part * 2].wait()
        for start in range(0, ROWS, LANES):
            x = jnp.concatenate(
                [
                    coh_ref[part, pol, k, :, start : min(start + LANES, PAIRS)].astype(F32)
                    for pol in range(2)
                    for k in range(16)
                ],
                axis=0,
            )
            if x.shape[1] < LANES:
                x = jnp.concatenate([x, jnp.zeros((LANES, LANES - x.shape[1]), F32)], axis=1)
            ct[part, start : start + LANES] = x.T
        for p in range(N):
            ct[part, p * N + p : p * N + p + 1] = jnp.zeros((1, LANES), F32)


def pair_sums(ct, vt, gain, total, weight, lhs, half, model):
    row = iota((256, LANES), 0) % LANES
    col = iota((256, LANES), 1)
    same = (row // 64 == col // 64) & (row % 4 == col % 4)
    adder = jnp.where(same, 1.0, 0.0).astype(BF16)

    def count(group):
        return min(GROUP, N - group * GROUP)

    def front(group):
        slot = group % 2
        for i in range(count(group)):
            p = group * GROUP + i
            c_real = ct[0, p * N : p * N + M]
            c_imag = ct[1, p * N : p * N + M]
            q_real = gain[:, :LANES]
            q_imag = gain[:, LANES:]
            h_real = c_real * q_real + c_imag * q_imag
            h_imag = c_imag * q_real - c_real * q_imag
            p_real = gain[p : p + 1, :LANES]
            p_imag = gain[p : p + 1, LANES:]
            half[slot, i * M : i * M + M, :LANES] = h_real
            half[slot, i * M : i * M + M, LANES:] = h_imag
            for at, m in (
                (i * 128, p_real * h_real - p_imag * h_imag),
                (i * 128 + M, p_real * h_imag + p_imag * h_real),
            ):
                high = m.astype(BF16)
                lhs[slot, at : at + M, :LANES] = high
                lhs[slot, at : at + M, LANES:] = (m - high.astype(F32)).astype(BF16)
        rows = count(group) * 128
        model[slot, :rows] = jnp.dot(lhs[slot, :rows], adder, preferred_element_type=F32)

    def back(group):
        slot = group % 2
        for i in range(count(group)):
            p = group * GROUP + i
            h_real = half[slot, i * M : i * M + M, :LANES]
            h_imag = half[slot, i * M : i * M + M, LANES:]
            d_real = vt[0, p * N : p * N + M] - model[slot, i * 128 : i * 128 + M]
            d_imag = vt[1, p * N : p * N + M] - model[slot, i * 128 + M : i * 128 + 128]

            def over_q(x):
                return jnp.sum(x, axis=0, keepdims=True)

            total[p : p + 1, :LANES] = over_q(d_real * h_real + d_imag * h_imag)
            total[p : p + 1, LANES:] = over_q(d_imag * h_real - d_real * h_imag)
            weight[p : p + 1] = over_q(h_real * h_real + h_imag * h_imag)

    total[N:] = jnp.zeros((M - N, 2 * LANES), F32)
    weight[N:] = jnp.zeros((M - N, LANES), F32)
    front(0)
    for group in range(M // GROUP):
        if group + 1 < M // GROUP:
            front(group + 1)
        back(group)


def solved(total, weight, gain, target):
    twice = jnp.concatenate([weight, weight], axis=1)
    return (total + gain * twice + penalty * target) / (twice + penalty)


def write_taps(card_ref, out_ref):
    card = card_ref[0]
    odd = lax.rem(card, 2) == 1
    source = iota((LANES, LANES), 0)
    target = iota((LANES, LANES), 1)
    lag = jnp.where(source // 4 == target // 4, source % 4 - target % 4, 100)

    def taps(shift):
        out = jnp.zeros((LANES, LANES), F32)
        for offset in range(-4, 5):
            out = jnp.where(lag + shift == offset, kernel_taps[offset + 4], out)
        return out

    after, before = taps(4), taps(-4)
    for i, weights in enumerate(
        (taps(0), jnp.where(odd, before, after), jnp.where(odd, after, before))
    ):
        high = weights.astype(BF16)
        low = (weights - high.astype(F32)).astype(BF16)
        out_ref[i * LANES : i * LANES + LANES] = high
        out_ref[(3 + i) * LANES : (4 + i) * LANES] = low


def first_kernel(
    coh_hbm, vis_hbm, jones_hbm, duals_hbm, card_ref,
    sum_ref, gain_ref, start_ref, duals_out, taps_ref, ct, vt,
    coh_ref, vis_ref, jones_ref, duals_ref, vflat, short, total, weight, lhs, half, model, arrived,
):
    copies = [
        pltpu.make_async_copy(source, target, arrived.at[i])
        for i, (source, target) in enumerate(
            [
                (jones_hbm, jones_ref),
                (duals_hbm, duals_ref),
                (vis_hbm, vis_ref),
                *((coh_hbm.at[a, b], coh_ref.at[a, b]) for a in range(2) for b in range(2)),
            ]
        )
    ]
    for copy in copies:
        copy.start()
    write_taps(card_ref, taps_ref)
    copies[0].wait()
    start_ref[...] = rows_first(jones_ref)
    copies[1].wait()
    duals_out[...] = rows_first(duals_ref)
    lay_out(coh_ref, vis_ref, vflat, short, ct, vt, copies[2:])
    pair_sums(ct, vt, start_ref, total, weight, lhs, half, model)
    gain = solved(total[...], weight[...], start_ref[...], start_ref[...] - duals_out[...])
    gain_ref[...] = gain
    sum_ref[...] = gain + duals_out[...]


def second_kernel(ct, vt, gain_ref, total, weight, lhs, half, model):
    pair_sums(ct, vt, gain_ref, total, weight, lhs, half, model)


def smoothed(taps_ref, own, inner, outer):
    x = jnp.concatenate(
        [
            jnp.concatenate([a[:, :LANES] for a in (own, inner, outer)], axis=1),
            jnp.concatenate([a[:, LANES:] for a in (own, inner, outer)], axis=1),
        ],
        axis=0,
    )
    high = x.astype(BF16)
    low = (x - high.astype(F32)).astype(BF16)

    def dot(a, b):
        return jnp.dot(a, b, preferred_element_type=F32)

    top, rest = taps_ref[: 3 * LANES], taps_ref[3 * LANES :]
    out = dot(high, top) + dot(low, top) + dot(high, rest)
    return jnp.concatenate([out[:M], out[M:]], axis=1)


def gaps(gain, fresh, consensus):
    primal = gain - fresh
    moved = fresh - consensus
    return (
        jnp.sum(primal * primal, keepdims=True),
        penalty * penalty * jnp.sum(moved * moved, keepdims=True),
    )


def third_kernel(
    taps_ref, own_ref, inner_ref, outer_ref, gain_ref, start_ref, duals_ref, total, weight,
    sum_ref, gain_out, fresh_ref, duals_out, norms_ref,
):
    fresh = smoothed(taps_ref, own_ref[...], inner_ref[...], outer_ref[...])
    gain = gain_ref[...]
    duals = duals_ref[...] + gain - fresh
    first, second = gaps(gain, fresh, start_ref[...])
    gain = solved(total[...], weight[...], gain, fresh - duals)
    gain_out[...] = gain
    fresh_ref[...] = fresh
    duals_out[...] = duals
    sum_ref[...] = gain + duals
    lane = iota((1, LANES), 1)
    norms_ref[...] = jnp.where(lane == 0, first, jnp.where(lane == 1, second, 0.0))


def fourth_kernel(
    taps_ref, own_ref, inner_ref, outer_ref, gain_ref, fresh_ref, duals_ref, norms_ref,
    fresh_out, duals_out, norms_out,
):
    fresh = smoothed(taps_ref, own_ref[...], inner_ref[...], outer_ref[...])
    gain = gain_ref[...]
    duals = duals_ref[...] + gain - fresh
    first, second = gaps(gain, fresh, fresh_ref[...])
    lane = iota((1, LANES), 1)
    norms = norms_ref[...] + jnp.where(lane == 2, first, jnp.where(lane == 3, second, 0.0))
    norms_out[...] = jnp.broadcast_to(norms[None], norms_out.shape)
    fresh_out[...] = fresh
    duals_out[...] = duals


def turn_kernel(*refs):
    for source, target in zip(refs[: len(refs) // 2], refs[len(refs) // 2 :]):
        rows_last(source[...], target)


def call(kernel, outs, ins, scratch=(), smem=(), hbm=(), flops=0):
    def space(i):
        return pltpu.SMEM if i in smem else pltpu.HBM if i in hbm else pltpu.VMEM

    return pl.pallas_call(
        kernel,
        out_shape=[
            jax.ShapeDtypeStruct(shape, F32) if isinstance(shape, tuple) else shape
            for shape in outs
        ],
        in_specs=[pl.BlockSpec(memory_space=space(i)) for i in range(len(ins))],
        out_specs=[pl.BlockSpec(memory_space=pltpu.VMEM) for _ in outs],
        scratch_shapes=scratch,
        cost_estimate=pl.CostEstimate(flops=flops, bytes_accessed=1000, transcendentals=0),
        compiler_params=pltpu.CompilerParams(vmem_limit_bytes=24 * 1024 * 1024),
    )(*ins)


def solve(visibility, coherency, jones_start, duals_start):
    cards = lax.axis_size("chan")
    entries = jones_start.size * cards
    card = lax.axis_index("chan").reshape(1)
    inner = [(i, i ^ 1) for i in range(cards)]
    outer = [(i, i - 1 if i % 2 == 0 else i + 1) for i in range(cards)]
    outer = [(a, b) for a, b in outer if 0 <= b < cards]
    state = (M, 2 * LANES)
    work = [
        pltpu.VMEM((2, GROUP * 128, 256), BF16),
        pltpu.VMEM((2, GROUP * M, 256), F32),
        pltpu.VMEM((2, GROUP * 128, LANES), F32),
    ]
    sums, gain, start, duals, taps, ct, vt = call(
        first_kernel,
        [
            state,
            state,
            state,
            state,
            jax.ShapeDtypeStruct((6 * LANES, LANES), BF16),
            (2, ROWS, LANES),
            (2, ROWS, LANES),
        ],
        (
            *(
                pltpu.with_memory_space_constraint(x, pltpu.HBM)
                for x in (
                    coherency.reshape(2, 2, 16, 4, PAIRS), visibility, jones_start, duals_start
                )
            ),
            card,
        ),
        [
            pltpu.VMEM((2, 2, 16, 4, PAIRS), BF16),
            pltpu.VMEM(visibility.shape, F32),
            pltpu.VMEM(jones_start.shape, F32),
            pltpu.VMEM(duals_start.shape, F32),
            pltpu.VMEM((48, ROWS), BF16),
            pltpu.VMEM((ROWS, 48), BF16),
            pltpu.VMEM(state, F32),
            pltpu.VMEM((M, LANES), F32),
            *work,
            pltpu.SemaphoreType.DMA((7,)),
        ],
        hbm=(0, 1, 2, 3),
        smem=(4,),
        flops=10**10,
    )

    def swapped(x):
        far = lax.ppermute(x, "chan", outer)
        near = lax.ppermute(x, "chan", inner)
        return near, far

    near, far = swapped(sums)
    total, weight = call(
        second_kernel, [state, (M, LANES)], (ct, vt, gain), work, flops=10**10
    )
    sums, gain, fresh, duals, norms = call(
        third_kernel,
        [state, state, state, state, (1, LANES)],
        (taps, sums, near, far, gain, start, duals, total, weight),
    )
    near, far = swapped(sums)
    shape = jones_start.shape
    (jones_now,) = call(turn_kernel, [shape], (gain,), flops=10**9)
    fresh, duals, norms = call(
        fourth_kernel,
        [state, state, (cards, 1, LANES)],
        (taps, sums, near, far, gain, fresh, duals, norms),
    )
    consensus, duals_now = call(turn_kernel, [shape, shape], (fresh, duals), flops=10**9)
    norms = lax.all_to_all(norms, "chan", split_axis=0, concat_axis=0, tiled=True)
    norms = jnp.sum(norms[:, 0, :4], axis=0).reshape(2, 2) / entries
    return jones_now, consensus, duals_now, norms


def solution(mesh):
    placed = (
        P(None, None, "chan", "slot", None),
        P(None, None, None, "chan", "slot", None),
        P(None, None, "slot", "chan", None),
        P(None, None, "slot", "chan", None),
    )
    return jax.shard_map(
        solve,
        mesh=mesh,
        in_specs=placed,
        out_specs=(
            P(None, None, "slot", "chan", None),
            P(None, None, "slot", "chan", None),
            P(None, None, "slot", "chan", None),
            P("slot", None),
        ),
        check_vma=False,
    )
```

```python
import jax
import jax.numpy as jnp
from jax import lax
from jax.experimental import pallas as pl
from jax.experimental.pallas import tpu as pltpu
from jax.sharding import PartitionSpec as P


penalty = 8.0
kernel_taps = (0.04, 0.06, 0.1, 0.15, 0.3, 0.15, 0.1, 0.06, 0.04)
N = 62
M = 64
LANES = 128
PAIRS = N * N
F32 = jnp.float32
BF16 = jnp.bfloat16
ROWS = 31 * LANES
GROUP = 4


def iota(shape, dim):
    return lax.broadcasted_iota(jnp.int32, shape, dim)


def rows_first(ref, out_rows=M):
    halves = []
    for part in range(2):
        x = jnp.concatenate([ref[part, pol, k] for pol in range(2) for k in range(16)], axis=0)
        x = jnp.concatenate([x, jnp.zeros((LANES, LANES - N), F32)], axis=1)
        halves.append(x.T[:out_rows])
    return jnp.concatenate(halves, axis=1)


def rows_last(x, ref):
    for part in range(2):
        half = x[:, part * LANES : (part + 1) * LANES]
        half = jnp.concatenate([half, jnp.zeros((LANES - M, LANES), F32)], axis=0).T
        for pol in range(2):
            for k in range(16):
                at = (pol * 16 + k) * 4
                ref[part, pol, k] = half[at : at + 4, :N]


def lay_out(coh_ref, vis_ref, vflat, short, ct, vt, copies):
    vflat[:, ROWS - LANES :] = jnp.zeros((48, LANES), BF16)
    copies[0].wait()
    v = jnp.concatenate(
        [vis_ref[a, b, f] for a in range(2) for b in range(2) for f in range(4)], axis=0
    )
    for split in range(3):
        high = v.astype(BF16)
        vflat[split * 16 : split * 16 + 16, :PAIRS] = high
        v = v - high.astype(F32)
    same = jnp.where(iota((LANES, LANES), 0) == iota((LANES, LANES), 1), 1.0, 0.0).astype(BF16)
    for start in range(0, ROWS, LANES):
        short[start : start + LANES] = lax.dot_general(
            same,
            vflat[:, start : start + LANES],
            (((1,), (1,)), ((), ())),
            preferred_element_type=F32,
        ).astype(BF16)
    source = iota((48, 256), 0)
    target = iota((48, 256), 1)
    spread = (
        ((source % 16) // 8 == target // LANES)
        & ((source % 8) // 4 == (target % LANES) // 64)
        & (source % 4 == target % 4)
    )
    spread = jnp.where(spread, 1.0, 0.0).astype(BF16)
    for part in range(2):
        copies[1 + part * 2].wait()
        copies[2 + part * 2].wait()
        for start in range(0, ROWS, LANES):
            x = jnp.concatenate(
                [
                    coh_ref[part, pol, k, :, start : min(start + LANES, PAIRS)].astype(F32)
                    for pol in range(2)
                    for k in range(16)
                ],
                axis=0,
            )
            if x.shape[1] < LANES:
                x = jnp.concatenate([x, jnp.zeros((LANES, LANES - x.shape[1]), F32)], axis=1)
            ct[part, start : start + LANES] = x.T
        for p in range(N):
            ct[part, p * N + p : p * N + p + 1] = jnp.zeros((1, LANES), F32)

    def widen(start):
        wide = jnp.dot(short[start : start + LANES], spread, preferred_element_type=F32)
        vt[0, start : start + LANES] = wide[:, :LANES]
        vt[1, start : start + LANES] = wide[:, LANES:]

    return widen


def pair_sums(ct, vt, gain, total, weight, lhs, half, model, widen=None):
    row = iota((256, LANES), 0) % LANES
    col = iota((256, LANES), 1)
    same = (row // 64 == col // 64) & (row % 4 == col % 4)
    adder = jnp.where(same, 1.0, 0.0)

    def count(group):
        return min(GROUP, N - group * GROUP)

    ready = [0]

    def front(group):
        slot = group % 2
        while widen and ready[0] < min((group * GROUP + count(group) - 1) * N + M, ROWS):
            widen(ready[0])
            ready[0] += LANES
        for i in range(count(group)):
            p = group * GROUP + i
            c_real = ct[0, p * N : p * N + M]
            c_imag = ct[1, p * N : p * N + M]
            q_real = gain[:, :LANES]
            q_imag = gain[:, LANES:]
            h_real = c_real * q_real + c_imag * q_imag
            h_imag = c_imag * q_real - c_real * q_imag
            p_real = gain[p : p + 1, :LANES]
            p_imag = gain[p : p + 1, LANES:]
            half[slot, i * M : i * M + M, :LANES] = h_real
            half[slot, i * M : i * M + M, LANES:] = h_imag
            for at, m in (
                (i * 128, p_real * h_real - p_imag * h_imag),
                (i * 128 + M, p_real * h_imag + p_imag * h_real),
            ):
                high = m.astype(BF16)
                lhs[slot, at : at + M, :LANES] = m
                lhs[slot, at : at + M, LANES:] = m - high.astype(F32)
        rows = count(group) * 128
        model[slot, :rows] = jnp.dot(
            lhs[slot, :rows], adder, precision=lax.Precision.DEFAULT, preferred_element_type=F32
        )

    def back(group):
        slot = group % 2
        for i in range(count(group)):
            p = group * GROUP + i
            h_real = half[slot, i * M : i * M + M, :LANES]
            h_imag = half[slot, i * M : i * M + M, LANES:]
            d_real = vt[0, p * N : p * N + M] - model[slot, i * 128 : i * 128 + M]
            d_imag = vt[1, p * N : p * N + M] - model[slot, i * 128 + M : i * 128 + 128]

            def over_q(x):
                return jnp.sum(x, axis=0, keepdims=True)

            total[p : p + 1, :LANES] = over_q(d_real * h_real + d_imag * h_imag)
            total[p : p + 1, LANES:] = over_q(d_imag * h_real - d_real * h_imag)
            weight[p : p + 1] = over_q(h_real * h_real + h_imag * h_imag)

    total[N:] = jnp.zeros((M - N, 2 * LANES), F32)
    weight[N:] = jnp.zeros((M - N, LANES), F32)
    front(0)
    for group in range(M // GROUP):
        if group + 1 < M // GROUP:
            front(group + 1)
        back(group)


def solved(total, weight, gain, target):
    twice = jnp.concatenate([weight, weight], axis=1)
    return (total + gain * twice + penalty * target) / (twice + penalty)


def write_taps(card_ref, out_ref):
    card = card_ref[0]
    odd = lax.rem(card, 2) == 1
    source = iota((LANES, LANES), 0)
    target = iota((LANES, LANES), 1)
    lag = jnp.where(source // 4 == target // 4, source % 4 - target % 4, 100)

    def taps(shift):
        out = jnp.zeros((LANES, LANES), F32)
        for offset in range(-4, 5):
            out = jnp.where(lag + shift == offset, kernel_taps[offset + 4], out)
        return out

    after, before = taps(4), taps(-4)
    for i, weights in enumerate(
        (taps(0), jnp.where(odd, before, after), jnp.where(odd, after, before))
    ):
        high = weights.astype(BF16)
        low = (weights - high.astype(F32)).astype(BF16)
        out_ref[i * LANES : i * LANES + LANES] = high
        out_ref[(3 + i) * LANES : (4 + i) * LANES] = low


def first_kernel(
    coh_hbm, vis_hbm, jones_hbm, duals_hbm, card_ref,
    sum_ref, gain_ref, start_ref, duals_out, taps_ref, ct, vt,
    coh_ref, vis_ref, jones_ref, duals_ref, vflat, short, total, weight, lhs, half, model, arrived,
):
    copies = [
        pltpu.make_async_copy(source, target, arrived.at[i])
        for i, (source, target) in enumerate(
            [
                (jones_hbm, jones_ref),
                (duals_hbm, duals_ref),
                (vis_hbm, vis_ref),
                *((coh_hbm.at[a, b], coh_ref.at[a, b]) for a in range(2) for b in range(2)),
            ]
        )
    ]
    for copy in copies:
        copy.start()
    write_taps(card_ref, taps_ref)
    copies[0].wait()
    start_ref[...] = rows_first(jones_ref)
    copies[1].wait()
    duals_out[...] = rows_first(duals_ref)
    widen = lay_out(coh_ref, vis_ref, vflat, short, ct, vt, copies[2:])
    pair_sums(ct, vt, start_ref, total, weight, lhs, half, model, widen)
    gain = solved(total[...], weight[...], start_ref[...], start_ref[...] - duals_out[...])
    gain_ref[...] = gain
    sum_ref[...] = gain + duals_out[...]


def second_kernel(ct, vt, gain_ref, total, weight, lhs, half, model):
    pair_sums(ct, vt, gain_ref, total, weight, lhs, half, model)


def smoothed(taps_ref, own, inner, outer):
    x = jnp.concatenate(
        [
            jnp.concatenate([a[:, :LANES] for a in (own, inner, outer)], axis=1),
            jnp.concatenate([a[:, LANES:] for a in (own, inner, outer)], axis=1),
        ],
        axis=0,
    )
    high = x.astype(BF16)
    low = (x - high.astype(F32)).astype(BF16)

    def dot(a, b):
        return jnp.dot(a, b, preferred_element_type=F32)

    top, rest = taps_ref[: 3 * LANES], taps_ref[3 * LANES :]
    out = dot(high, top) + dot(low, top) + dot(high, rest)
    return jnp.concatenate([out[:M], out[M:]], axis=1)


def gaps(gain, fresh, consensus):
    primal = gain - fresh
    moved = fresh - consensus
    return (
        jnp.sum(primal * primal, keepdims=True),
        penalty * penalty * jnp.sum(moved * moved, keepdims=True),
    )


def third_kernel(
    taps_ref, own_ref, inner_ref, outer_ref, gain_ref, start_ref, duals_ref, total, weight,
    sum_ref, gain_out, fresh_ref, duals_out, norms_ref,
):
    fresh = smoothed(taps_ref, own_ref[...], inner_ref[...], outer_ref[...])
    gain = gain_ref[...]
    duals = duals_ref[...] + gain - fresh
    first, second = gaps(gain, fresh, start_ref[...])
    gain = solved(total[...], weight[...], gain, fresh - duals)
    gain_out[...] = gain
    fresh_ref[...] = fresh
    duals_out[...] = duals
    sum_ref[...] = gain + duals
    lane = iota((1, LANES), 1)
    norms_ref[...] = jnp.where(lane == 0, first, jnp.where(lane == 1, second, 0.0))


def fourth_kernel(
    taps_ref, own_ref, inner_ref, outer_ref, gain_ref, fresh_ref, duals_ref, norms_ref,
    fresh_out, duals_out, norms_out,
):
    fresh = smoothed(taps_ref, own_ref[...], inner_ref[...], outer_ref[...])
    gain = gain_ref[...]
    duals = duals_ref[...] + gain - fresh
    first, second = gaps(gain, fresh, fresh_ref[...])
    lane = iota((1, LANES), 1)
    norms = norms_ref[...] + jnp.where(lane == 2, first, jnp.where(lane == 3, second, 0.0))
    norms_out[...] = jnp.broadcast_to(norms[None], norms_out.shape)
    fresh_out[...] = fresh
    duals_out[...] = duals


def turn_kernel(*refs):
    for source, target in zip(refs[: len(refs) // 2], refs[len(refs) // 2 :]):
        rows_last(source[...], target)


def call(kernel, outs, ins, scratch=(), smem=(), hbm=(), flops=0):
    def space(i):
        return pltpu.SMEM if i in smem else pltpu.HBM if i in hbm else pltpu.VMEM

    return pl.pallas_call(
        kernel,
        out_shape=[
            jax.ShapeDtypeStruct(shape, F32) if isinstance(shape, tuple) else shape
            for shape in outs
        ],
        in_specs=[pl.BlockSpec(memory_space=space(i)) for i in range(len(ins))],
        out_specs=[pl.BlockSpec(memory_space=pltpu.VMEM) for _ in outs],
        scratch_shapes=scratch,
        cost_estimate=pl.CostEstimate(flops=flops, bytes_accessed=1000, transcendentals=0),
        compiler_params=pltpu.CompilerParams(vmem_limit_bytes=24 * 1024 * 1024),
    )(*ins)


def solve(visibility, coherency, jones_start, duals_start):
    cards = lax.axis_size("chan")
    entries = jones_start.size * cards
    card = lax.axis_index("chan").reshape(1)
    inner = [(i, i ^ 1) for i in range(cards)]
    outer = [(i, i - 1 if i % 2 == 0 else i + 1) for i in range(cards)]
    outer = [(a, b) for a, b in outer if 0 <= b < cards]
    state = (M, 2 * LANES)
    work = [
        pltpu.VMEM((2, GROUP * 128, 256), F32),
        pltpu.VMEM((2, GROUP * M, 256), F32),
        pltpu.VMEM((2, GROUP * 128, LANES), F32),
    ]
    sums, gain, start, duals, taps, ct, vt = call(
        first_kernel,
        [
            state,
            state,
            state,
            state,
            jax.ShapeDtypeStruct((6 * LANES, LANES), BF16),
            (2, ROWS, LANES),
            (2, ROWS, LANES),
        ],
        (
            *(
                pltpu.with_memory_space_constraint(x, pltpu.HBM)
                for x in (
                    coherency.reshape(2, 2, 16, 4, PAIRS), visibility, jones_start, duals_start
                )
            ),
            card,
        ),
        [
            pltpu.VMEM((2, 2, 16, 4, PAIRS), BF16),
            pltpu.VMEM(visibility.shape, F32),
            pltpu.VMEM(jones_start.shape, F32),
            pltpu.VMEM(duals_start.shape, F32),
            pltpu.VMEM((48, ROWS), BF16),
            pltpu.VMEM((ROWS, 48), BF16),
            pltpu.VMEM(state, F32),
            pltpu.VMEM((M, LANES), F32),
            *work,
            pltpu.SemaphoreType.DMA((7,)),
        ],
        hbm=(0, 1, 2, 3),
        smem=(4,),
        flops=10**10,
    )

    def swapped(x):
        far = lax.ppermute(x, "chan", outer)
        near = lax.ppermute(x, "chan", inner)
        return near, far

    near, far = swapped(sums)
    total, weight = call(
        second_kernel, [state, (M, LANES)], (ct, vt, gain), work, flops=10**10
    )
    sums, gain, fresh, duals, norms = call(
        third_kernel,
        [state, state, state, state, (1, LANES)],
        (taps, sums, near, far, gain, start, duals, total, weight),
    )
    near, far = swapped(sums)
    shape = jones_start.shape
    (jones_now,) = call(turn_kernel, [shape], (gain,), flops=10**9)
    fresh, duals, norms = call(
        fourth_kernel,
        [state, state, (cards, 1, LANES)],
        (taps, sums, near, far, gain, fresh, duals, norms),
    )
    consensus, duals_now = call(turn_kernel, [shape, shape], (fresh, duals), flops=10**9)
    norms = lax.all_to_all(norms, "chan", split_axis=0, concat_axis=0, tiled=True)
    norms = jnp.sum(norms[:, 0, :4], axis=0).reshape(2, 2) / entries
    return jones_now, consensus, duals_now, norms


def solution(mesh):
    placed = (
        P(None, None, "chan", "slot", None),
        P(None, None, None, "chan", "slot", None),
        P(None, None, "slot", "chan", None),
        P(None, None, "slot", "chan", None),
    )
    return jax.shard_map(
        solve,
        mesh=mesh,
        in_specs=placed,
        out_specs=(
            P(None, None, "slot", "chan", None),
            P(None, None, "slot", "chan", None),
            P(None, None, "slot", "chan", None),
            P("slot", None),
        ),
        check_vma=False,
    )
```
